32 devices in a mesh: dp: 4 (over y, z), ep: 8 (over x, core).
Axes of the slice: x: 4, y: 2, z: 2, core: 2. Of those that a mesh axis runs over, the one named last changes fastest.
The devices are a block of a 4x4x8 slice.
Arguments:
- x_disp: bfloat16 [32, 32, 192, 1024], P('dp', 'ep'), parts along dimension 0
- w_gate: bfloat16 [32, 1024, 512], P('ep')
- w_up: bfloat16 [32, 1024, 512], P('ep')
- w_down: bfloat16 [32, 512, 1024], P('ep')
- d_out: bfloat16 [12288, 1024], P(('dp', 'ep')), parts along dimension 0
- slot_idx: int32 [12288, 8], P(('dp', 'ep')), parts along dimension 0
- expert_id: int32 [12288, 8], P(('dp', 'ep')), parts along dimension 0
- gate_wt: float32 [12288, 8], P(('dp', 'ep')), parts along dimension 0
Outputs:
- output 1: bfloat16 [32, 32, 192, 1024], P('dp', 'ep'), parts along dimension 0
- output 2: bfloat16 [128, 1024, 512], P(('dp', 'ep')), parts along dimension 0
- output 3: bfloat16 [128, 1024, 512], P(('dp', 'ep')), parts along dimension 0
- output 4: bfloat16 [128, 512, 1024], P(('dp', 'ep')), parts along dimension 0
- output 5: float32 [12288, 8], P(('dp', 'ep')), parts along dimension 0
There are 4 independent parts. The reference program is written for one: setup_inputs(seed, part) draws one part's arguments, and reference() takes and returns one part's arrays. A program takes and returns all parts, laid end to end along the dimension named above; an argument that names none is the same for every part.
All inputs are finite; a program needn't handle non-finite values.
Results may differ from the reference program's by a relative error of at most 0.00499497.
Values are sent between devices in bfloat16 or wider.
A program may use at most 768 MiB of HBM per device.

```python
import jax
import jax.numpy as jnp
from jax import lax

GROUP_SIZE = 8
TOK_DEV = 384
TOP_K = 8
EXPERTS = 32
MODEL_DIM = 1024
FFN_DIM = 512
CAPACITY = 192

TOKENS = GROUP_SIZE * TOK_DEV
SLOT_COUNT = EXPERTS * CAPACITY
PER_SOURCE = TOK_DEV * TOP_K


def draw_routes(key):
    key_noise, key_tilt, key_hot = jax.random.split(key, 3)
    noise_int = jax.random.randint(key_noise, (TOKENS, EXPERTS), 0, 4096)
    tilt_int = jax.random.permutation(key_tilt, EXPERTS) * (1024 // EXPERTS)
    hot_expert = jax.random.randint(key_hot, (), 0, EXPERTS)
    expert_ids = jnp.arange(EXPERTS)[None, :]
    even_tok = (jnp.arange(TOKENS) % 2 == 0)[:, None]
    bonus_int = jnp.where(even_tok & (expert_ids == hot_expert), 1048576, 0)
    scores = (noise_int + tilt_int[None, :] + bonus_int) * EXPERTS + expert_ids
    expert_id = lax.top_k(scores, TOP_K)[1].astype(jnp.int32)
    picked = jnp.zeros((TOKENS, EXPERTS), jnp.int32).at[jnp.arange(TOKENS)[:, None], expert_id].add(1)
    picked = picked.reshape(GROUP_SIZE, TOK_DEV, EXPERTS)
    earlier = jnp.cumsum(picked, axis=1) - picked
    order_pos = jnp.take_along_axis(earlier, expert_id.reshape(GROUP_SIZE, TOK_DEV, TOP_K), axis=2)
    slot_idx = jnp.where(order_pos < CAPACITY, order_pos, -1).reshape(TOKENS, TOP_K).astype(jnp.int32)
    return slot_idx, expert_id


def setup_inputs(seed: int = 0, part: int = 0) -> dict:
    base_key = jax.random.key(seed)
    part_key = jax.random.fold_in(base_key, part)
    key_x, key_out, key_gate, key_route = jax.random.split(part_key, 4)
    key_wg, key_wu, key_wd = jax.random.split(jax.random.key(seed + 1), 3)
    x_disp = jax.random.normal(key_x, (GROUP_SIZE, EXPERTS, CAPACITY, MODEL_DIM), jnp.float32).astype(jnp.bfloat16)
    w_gate = (jax.random.normal(key_wg, (EXPERTS, MODEL_DIM, FFN_DIM), jnp.float32) * MODEL_DIM ** -0.5).astype(jnp.bfloat16)
    w_up = (jax.random.normal(key_wu, (EXPERTS, MODEL_DIM, FFN_DIM), jnp.float32) * MODEL_DIM ** -0.5).astype(jnp.bfloat16)
    w_down = (jax.random.normal(key_wd, (EXPERTS, FFN_DIM, MODEL_DIM), jnp.float32) * FFN_DIM ** -0.5).astype(jnp.bfloat16)
    d_out = jax.random.normal(key_out, (TOKENS, MODEL_DIM), jnp.float32).astype(jnp.bfloat16)
    slot_idx, expert_id = draw_routes(key_route)
    gate_wt = jax.random.uniform(key_gate, (TOKENS, TOP_K), jnp.float32, 0.05, 1.0)
    return {'x_disp': x_disp, 'w_gate': w_gate, 'w_up': w_up, 'w_down': w_down, 'd_out': d_out, 'slot_idx': slot_idx, 'expert_id': expert_id, 'gate_wt': gate_wt}


def one_expert(operands):
    x_rows, out_rows, d_slot, w_gate, w_up, w_down = operands
    pre_gate = jnp.dot(x_rows, w_gate, preferred_element_type=jnp.float32)
    pre_up = jnp.dot(x_rows, w_up, preferred_element_type=jnp.float32)
    gate_sig = jax.nn.sigmoid(pre_gate)
    silu_gate = pre_gate * gate_sig
    hidden = (silu_gate * pre_up).astype(jnp.bfloat16)
    y_rows = jnp.dot(hidden, w_down, preferred_element_type=jnp.float32).astype(jnp.bfloat16)
    grad_hidden = jnp.dot(d_slot, w_down.T, preferred_element_type=jnp.float32).astype(jnp.bfloat16).astype(jnp.float32)
    grad_pre_gate = (grad_hidden * pre_up * gate_sig * (1.0 + pre_gate * (1.0 - gate_sig))).astype(jnp.bfloat16)
    grad_pre_up = (grad_hidden * silu_gate).astype(jnp.bfloat16)
    grad_x = (jnp.dot(grad_pre_gate, w_gate.T, preferred_element_type=jnp.float32) + jnp.dot(grad_pre_up, w_up.T, preferred_element_type=jnp.float32)).astype(jnp.bfloat16)
    grad_w_gate = jnp.dot(x_rows.T, grad_pre_gate, preferred_element_type=jnp.float32).astype(jnp.bfloat16)
    grad_w_up = jnp.dot(x_rows.T, grad_pre_up, preferred_element_type=jnp.float32).astype(jnp.bfloat16)
    grad_w_down = jnp.dot(hidden.T, d_slot, preferred_element_type=jnp.float32).astype(jnp.bfloat16)
    gate_grad_rows = jnp.sum(out_rows.astype(jnp.float32) * y_rows.astype(jnp.float32), axis=1)
    return grad_x, grad_w_gate, grad_w_up, grad_w_down, gate_grad_rows


def by_expert(arr):
    return jnp.moveaxis(arr.reshape(GROUP_SIZE, EXPERTS, CAPACITY, MODEL_DIM), 1, 0).reshape(EXPERTS, GROUP_SIZE * CAPACITY, MODEL_DIM)


def owners(pos_row):
    return jnp.full((SLOT_COUNT,), PER_SOURCE, jnp.int32).at[pos_row].set(jnp.arange(PER_SOURCE, dtype=jnp.int32), mode='drop')


def pick_rows(tok_rows, gate_row, owner_row):
    rows_out = jnp.take(tok_rows, owner_row // TOP_K, axis=0, mode='fill', fill_value=0)
    gates_out = jnp.take(gate_row, owner_row, mode='fill', fill_value=0)
    return rows_out, gates_out


def take_fill(values, index_row):
    return jnp.take(values, index_row, mode='fill', fill_value=0)


def reference(x_disp, w_gate, w_up, w_down, d_out, slot_idx, expert_id, gate_wt):
    flat_pos = jnp.where(slot_idx >= 0, expert_id * CAPACITY + slot_idx, SLOT_COUNT).reshape(GROUP_SIZE, PER_SOURCE)
    owner_ids = jax.vmap(owners)(flat_pos)
    out_rows, gate_rows = jax.vmap(pick_rows)(d_out.reshape(GROUP_SIZE, TOK_DEV, MODEL_DIM), gate_wt.reshape(GROUP_SIZE, PER_SOURCE), owner_ids)
    d_slot = (out_rows.astype(jnp.float32) * gate_rows[:, :, None]).astype(jnp.bfloat16)
    results = lax.map(one_expert, (by_expert(x_disp), by_expert(out_rows), by_expert(d_slot), w_gate, w_up, w_down))
    grad_x, grad_w_gate, grad_w_up, grad_w_down, gate_grad_rows = results
    grad_x_disp = jnp.moveaxis(grad_x.reshape(EXPERTS, GROUP_SIZE, CAPACITY, MODEL_DIM), 0, 1)
    gate_grad_src = jnp.moveaxis(gate_grad_rows.reshape(EXPERTS, GROUP_SIZE, CAPACITY), 0, 1).reshape(GROUP_SIZE, SLOT_COUNT)
    grad_gate = jax.vmap(take_fill)(gate_grad_src, flat_pos).reshape(TOKENS, TOP_K)
    return grad_x_disp, grad_w_gate, grad_w_up, grad_w_down, grad_gate
```

```python
import functools

import jax
import jax.numpy as jnp
from jax import lax
from jax.experimental import pallas as pl
from jax.experimental.pallas import tpu as pltpu
from jax.sharding import PartitionSpec as P

BF16 = jnp.bfloat16
F32 = jnp.float32
MESH = pl.DeviceIdType.MESH
NT = (((1,), (1,)), ((), ()))
TN = (((0,), (0,)), ((), ()))


def slot_kernel(x_hbm, wg_hbm, wu_hbm, wd_hbm, d_hbm, slot_in, exp_in, gate_in,
                h_hbm, ab_hbm, dy_hbm, gg_ref, cnt_ref,
                d_all, f1, f2, hid, m_slot, m_exp, m_gate, xb, wgb, wub, wdb, dbuf, dyb, abb,
                x_sem, w_sem, wd_sem, own_sem, h_sem, out_sem,
                link_send, link_recv, meta_send, meta_recv):
    chips, cores = 4, 2
    e_local, cap = x_hbm.shape[1], x_hbm.shape[2]
    tok, ffn = d_hbm.shape[0], wg_hbm.shape[2]
    half = tok // 2
    blocks = chips * e_local
    me = lax.axis_index('ep')
    chip, core = me // cores, me % cores
    right = lax.rem(chip + 1, chips)
    left = lax.rem(chip + chips - 1, chips)
    far = lax.rem(chip + 2, chips)
    to_right, to_left, to_sib = right * cores + core, left * cores + core, chip * cores + (1 - core)

    def x_copy(i, slot, k):
        return pltpu.make_async_copy(x_hbm.at[(i % chips) * cores + k, i // chips], xb.at[slot, pl.ds(k * cap, cap)], x_sem.at[slot, k])

    def w_copies(e, slot):
        return (pltpu.make_async_copy(wg_hbm.at[e], wgb.at[slot], w_sem.at[slot, 0]),
                pltpu.make_async_copy(wu_hbm.at[e], wub.at[slot], w_sem.at[slot, 1]))

    def rows(h):
        return pl.ds(h * half, half)

    def link(src_ref, s, h, dst, n):
        return pltpu.make_async_remote_copy(src_ref=src_ref, dst_ref=d_all.at[s, rows(h)], send_sem=link_send.at[n],
                                            recv_sem=link_recv.at[s, h], device_id={'ep': dst}, device_id_type=MESH)

    def meta(k, other, s):
        src, dst = ((slot_in, m_slot), (exp_in, m_exp), (gate_in, m_gate))[k]
        return pltpu.make_async_remote_copy(src_ref=src, dst_ref=dst.at[s], send_sem=meta_send.at[k, other],
                                            recv_sem=meta_recv.at[k, s], device_id={'ep': other}, device_id_type=MESH)

    def got(s, h):
        link(d_hbm.at[rows(h)], s, h, to_sib, 0).wait_recv()

    for c in w_copies(0, 0):
        c.start()
    for k in range(cores):
        x_copy(0, 0, k).start()
    own_copy = pltpu.make_async_copy(d_hbm, d_all.at[me], own_sem)
    own_copy.start()
    wd_copy = pltpu.make_async_copy(wd_hbm, wdb, wd_sem)

    barrier = pltpu.get_barrier_semaphore()
    n_dev = chips * cores

    def greet(k, carry):
        pl.semaphore_signal(barrier, inc=1, device_id={'ep': lax.rem(me + k, n_dev)}, device_id_type=MESH)
        return carry
    lax.fori_loop(1, n_dev, greet, 0)
    pl.semaphore_wait(barrier, n_dev - 1)

    own_links = [link(d_hbm.at[rows(h)], me, h, dst, n) for n, (dst, h) in enumerate(
        ((to_right, 0), (to_left, 1), (to_right, 1), (to_left, 0), (to_sib, 0), (to_sib, 1)))]

    def send_meta(k, carry):
        for a in range(3):
            meta(a, lax.rem(me + k, n_dev), me).start()
        return carry
    lax.fori_loop(1, n_dev, send_meta, 0)
    for c in own_links:
        c.start()
    wd_copy.start()
    m_slot[me] = slot_in[...]
    m_exp[me] = exp_in[...]
    m_gate[me] = gate_in[...]

    l_src, r_src, f_src = left * cores + core, right * cores + core, far * cores + core
    pass_on = [link(d_all.at[l_src, rows(0)], l_src, 0, to_right, 6), link(d_all.at[r_src, rows(1)], r_src, 1, to_left, 7)]
    share = [link(d_all.at[s, rows(h)], s, h, to_sib, 8 + n) for n, (s, h) in enumerate(
        ((l_src, 0), (r_src, 1), (r_src, 0), (l_src, 1), (f_src, 0), (f_src, 1)))]

    def forward(i, carry):
        slot = i % 2
        e = i // chips

        @pl.when(i + 1 < blocks)
        def _():
            for k in range(cores):
                x_copy(i + 1, 1 - slot, k).start()

        @pl.when(i % chips == 0)
        def _():
            for c in w_copies(e, e % 2):
                c.wait()

            @pl.when(e + 1 < e_local)
            def _():
                for c in w_copies(e + 1, (e + 1) % 2):
                    c.start()

        for k in range(cores):
            x_copy(i, slot, k).wait()

        @pl.when(i == 10)
        def _():
            got(l_src, 0)
            pass_on[0].start()
            got(r_src, 1)
            pass_on[1].start()
            share[0].start()
            share[1].start()

        x = xb[slot]
        for n in range(0, ffn, 256):
            a = jnp.dot(x, wgb[e % 2, :, n:n + 256], preferred_element_type=F32)
            b = jnp.dot(x, wub[e % 2, :, n:n + 256], preferred_element_type=F32)
            sg = jax.nn.sigmoid(a)
            silu = a * sg
            f1[i, :, n:n + 256] = b * sg * (1.0 + a * (1.0 - sg))
            f2[i, :, n:n + 256] = silu
            hid[i, :, n:n + 256] = (silu * b).astype(BF16)
        for k in range(cores):
            h_copy(i, k).start()
        return carry

    def h_copy(i, k):
        return pltpu.make_async_copy(hid.at[i, pl.ds(k * cap, cap)], h_hbm.at[(i % chips) * cores + k, i // chips], h_sem.at[i, k])

    lax.fori_loop(0, blocks, forward, 0)

    own_copy.wait()
    wd_copy.wait()

    def got_meta(k, carry):
        s = lax.rem(me + k, n_dev)
        for a in range(3):
            meta(a, s, s).wait_recv()
        return carry
    lax.fori_loop(1, n_dev, got_meta, 0)
    sib = to_sib
    got(sib, 0)
    got(sib, 1)

    cap_ids = lax.broadcasted_iota(jnp.int32, (cap, tok), 0)

    def place(q):
        g, e = q // e_local, q % e_local
        return lax.rem(chip + g + (g // 2) * (5 - 2 * g), chips), e

    def out_copies(q, slot):
        p, e = place(q)
        return [pltpu.make_async_copy(buf.at[slot, pl.ds(k * cap, cap)], dst.at[p * cores + k, e], out_sem.at[slot, j, k])
                for j, (buf, dst) in enumerate(((dyb, dy_hbm), (abb, ab_hbm))) for k in range(cores)]

    def backward(q, carry):
        slot = q % 2
        p, e = place(q)
        i = e * chips + p

        @pl.when(q == e_local)
        def _():
            got(r_src, 0)
            share[2].start()
            got(l_src, 1)
            share[3].start()
            for s in (right * cores + 1 - core, left * cores + 1 - core):
                got(s, 0)
                got(s, 1)

        @pl.when(q == 3 * e_local)
        def _():
            got(f_src, 0)
            share[4].start()
            got(f_src, 1)
            share[5].start()
            for h in range(2):
                got(far * cores + 1 - core, h)

        @pl.when(q >= 2)
        def _():
            for c in out_copies(q - 2, slot):
                c.wait()

        eid = me * e_local + e
        hits, gates = [], []
        for k in range(cores):
            s = p * cores + k
            slots = m_slot[s]
            match = (m_exp[s] == eid) & (slots >= 0)
            at = jnp.sum(jnp.where(match, slots + 1, 0), axis=0, keepdims=True) - 1
            gate = jnp.sum(jnp.where(match, m_gate[s], 0.0), axis=0, keepdims=True)
            cnt_ref[s * e_local + e] = jnp.sum(jnp.where(match, 1, 0))
            hit = cap_ids == at
            gcol = jnp.sum(jnp.where(hit, gate, 0.0), axis=1, keepdims=True)
            d = jnp.dot(jnp.where(hit, 1.0, 0.0).astype(BF16), d_all[s], preferred_element_type=F32)
            dbuf[k * cap:(k + 1) * cap] = d.astype(BF16)
            dyb[slot, k * cap:(k + 1) * cap] = (d * gcol).astype(BF16)
            hits.append(hit)
            gates.append(gcol)
        gcol = jnp.concatenate(gates, axis=0)
        dot_h = jnp.zeros((cores * cap, 1), F32)
        for n in range(0, ffn, 256):
            u = lax.dot_general(dbuf[...], wdb[e, n:n + 256, :], NT, preferred_element_type=F32)
            dot_h = dot_h + jnp.sum(u * hid[i, :, n:n + 256].astype(F32), axis=1, keepdims=True)
            dh = (u * gcol).astype(BF16).astype(F32)
            abb[slot, :, n:n + 256] = (dh * f1[i, :, n:n + 256]).astype(BF16)
            abb[slot, :, ffn + n:ffn + n + 256] = (dh * f2[i, :, n:n + 256]).astype(BF16)
        for k in range(cores):
            s = p * cores + k
            gg_ref[s * e_local + e] = jnp.sum(jnp.where(hits[k], dot_h[k * cap:(k + 1) * cap], 0.0), axis=0, keepdims=True)
        for c in out_copies(q, slot):
            c.start()
        return carry

    lax.fori_loop(0, blocks, backward, 0)
    for q in (blocks - 2, blocks - 1):
        for c in out_copies(q, q % 2):
            c.wait()

    def h_done(i, carry):
        for k in range(cores):
            h_copy(i, k).wait()
        return carry
    lax.fori_loop(0, blocks, h_done, 0)

    def meta_done(k, carry):
        for a in range(3):
            meta(a, lax.rem(me + k, n_dev), me).wait_send()
        return carry
    lax.fori_loop(1, n_dev, meta_done, 0)
    for c in own_links + pass_on + share:
        c.wait_send()


def slot_call(x_disp, w_gate, w_up, w_down, d_out, slot_t, exp_t, gate_t):
    n_src, e_local, cap, dim = x_disp.shape
    ffn = w_gate.shape[2]
    tok, top_k = d_out.shape[0], slot_t.shape[0]
    blocks = n_src // 2 * e_local
    hbm = pl.BlockSpec(memory_space=pl.ANY)
    vmem = pl.BlockSpec(memory_space=pltpu.VMEM)
    smem = pl.BlockSpec(memory_space=pltpu.SMEM)
    dma = pltpu.SemaphoreType.DMA
    return pl.pallas_call(
        slot_kernel,
        out_shape=(jax.ShapeDtypeStruct((n_src, e_local, cap, ffn), BF16),
                   jax.ShapeDtypeStruct((n_src, e_local, cap, 2 * ffn), BF16),
                   jax.ShapeDtypeStruct((n_src, e_local, cap, dim), BF16),
                   jax.ShapeDtypeStruct((n_src * e_local, 1, tok), F32),
                   jax.ShapeDtypeStruct((n_src * e_local,), jnp.int32)),
        in_specs=[hbm] * 5 + [vmem] * 3,
        out_specs=(hbm, hbm, hbm, vmem, smem),
        scratch_shapes=[
            pltpu.VMEM((n_src, tok, dim), BF16),
            pltpu.VMEM((blocks, 2 * cap, ffn), F32), pltpu.VMEM((blocks, 2 * cap, ffn), F32),
            pltpu.VMEM((blocks, 2 * cap, ffn), BF16),
            pltpu.VMEM((n_src, top_k, tok), jnp.int32), pltpu.VMEM((n_src, top_k, tok), jnp.int32), pltpu.VMEM((n_src, top_k, tok), F32),
            pltpu.VMEM((2, 2 * cap, dim), BF16),
            pltpu.VMEM((2, dim, ffn), BF16), pltpu.VMEM((2, dim, ffn), BF16), pltpu.VMEM((e_local, ffn, dim), BF16),
            pltpu.VMEM((2 * cap, dim), BF16), pltpu.VMEM((2, 2 * cap, dim), BF16), pltpu.VMEM((2, 2 * cap, 2 * ffn), BF16),
            dma((2, 2)), dma((2, 2)), dma, dma, dma((blocks, 2)), dma((2, 2, 2)),
            dma((14,)), dma((n_src, 2)), dma((3, n_src)), dma((3, n_src)),
        ],
        compiler_params=pltpu.CompilerParams(collective_id=0, has_side_effects=True, vmem_limit_bytes=62 * 1024 * 1024),
        cost_estimate=pl.CostEstimate(flops=8 * n_src * e_local * cap * dim * ffn, bytes_accessed=64 * 2 ** 20, transcendentals=0),
        name='slot_cotangents',
    )(x_disp, w_gate, w_up, w_down, d_out, slot_t, exp_t, gate_t)


def grad_kernel(cnt, x_hbm, ab_hbm, h_hbm, dy_hbm, wg_hbm, wu_hbm,
                dx_hbm, dwg_hbm, dwu_hbm, dwd_hbm,
                xb, abb, hb, dyb, wgb, wub, dxb, dwgb, dwub, dwdb, zeros,
                in_sem, w_sem, dx_sem, z_sem, dw_sem):
    n_src, e_local, cap, dim = x_hbm.shape
    ffn = wg_hbm.shape[2]
    step, grain = 256, 16
    pairs = ((x_hbm, xb), (ab_hbm, abb), (h_hbm, hb), (dy_hbm, dyb))

    def spans(e):
        out, start = [], jnp.int32(0)
        for s in range(n_src):
            n = (cnt[s * e_local + e] + (grain - 1)) // grain * grain
            out.append((pl.multiple_of(start, grain), pl.multiple_of(n, grain)))
            start = start + n
        return out, pl.multiple_of(start, grain)

    def loads(e, slot, do):
        for s, (start, n) in enumerate(spans(e)[0]):
            @pl.when(n > 0)
            def _():
                for j, (src, dst) in enumerate(pairs):
                    do(pltpu.make_async_copy(src.at[s, e, pl.ds(0, n)], dst.at[slot, pl.ds(start, n)], in_sem.at[slot, j, s]))
        do(pltpu.make_async_copy(wg_hbm.at[e], wgb.at[slot], w_sem.at[slot, 0]))
        do(pltpu.make_async_copy(wu_hbm.at[e], wub.at[slot], w_sem.at[slot, 1]))

    def dx_stores(e, slot, do):
        for s, (start, n) in enumerate(spans(e)[0]):
            @pl.when(n > 0)
            def _():
                do(pltpu.make_async_copy(dxb.at[slot, pl.ds(start, n)], dx_hbm.at[s, e, pl.ds(0, n)], dx_sem.at[slot, s]))

    def zero_stores(e, do):
        for s, (_, n) in enumerate(spans(e)[0]):
            rest = pl.multiple_of(cap - n, grain)

            @pl.when(rest > 0)
            def _():
                do(pltpu.make_async_copy(zeros.at[pl.ds(0, rest)], dx_hbm.at[s, e, pl.ds(n, rest)], z_sem.at[s]))

    def dw_stores(e, slot, do):
        for j, (src, dst) in enumerate(((dwgb, dwg_hbm), (dwub, dwu_hbm), (dwdb, dwd_hbm))):
            do(pltpu.make_async_copy(src.at[slot], dst.at[e], dw_sem.at[slot, j]))

    start = lambda c: c.start()
    wait = lambda c: c.wait()

    loads(0, 0, start)
    zeros[...] = jnp.zeros_like(zeros)

    def expert(e, carry):
        slot = e % 2

        @pl.when(e + 1 < e_local)
        def _():
            loads(e + 1, 1 - slot, start)

        @pl.when(e > 0)
        def _():
            zero_stores(e - 1, wait)
        zero_stores(e, start)
        loads(e, slot, wait)

        @pl.when(e >= 2)
        def _():
            dx_stores(e - 2, slot, wait)
            dw_stores(e - 2, slot, wait)

        total = spans(e)[1]
        count = jnp.maximum((total + (step - 1)) // step, 1)

        def clear(j, c):
            at = pl.ds(pl.multiple_of(total + j * grain, grain), grain)
            for buf in (xb, abb, hb, dyb):
                buf[slot, at, :] = jnp.zeros((grain, buf.shape[2]), BF16)
            return c
        lax.fori_loop(0, (count * step - total) // grain, clear, 0)

        for k in range(1, n_src * cap // step + 1):
            rows = k * step

            @pl.when(count == k)
            def _():
                def dx_tile(n, c):
                    at = pl.ds(pl.multiple_of(n * 256, 256), 256)
                    dxb[slot, :rows, at] = (
                        lax.dot_general(abb[slot, :rows, :ffn], wgb[slot, at, :], NT, preferred_element_type=F32)
                        + lax.dot_general(abb[slot, :rows, ffn:], wub[slot, at, :], NT, preferred_element_type=F32)).astype(BF16)
                    return c
                lax.fori_loop(0, dim // 256, dx_tile, 0)

                def up_tile(m, c):
                    at = pl.ds(pl.multiple_of(m * 256, 256), 256)
                    r = lax.dot_general(xb[slot, :rows, at], abb[slot, :rows, :], TN, preferred_element_type=F32).astype(BF16)
                    dwgb[slot, at, :] = r[:, :ffn]
                    dwub[slot, at, :] = r[:, ffn:]
                    return c
                lax.fori_loop(0, dim // 256, up_tile, 0)

                def down_tile(m, c):
                    at = pl.ds(pl.multiple_of(m * 256, 256), 256)
                    dwdb[slot, at, :] = lax.dot_general(hb[slot, :rows, at], dyb[slot, :rows, :], TN, preferred_element_type=F32).astype(BF16)
                    return c
                lax.fori_loop(0, ffn // 256, down_tile, 0)

        dx_stores(e, slot, start)
        dw_stores(e, slot, start)
        return carry

    lax.fori_loop(0, e_local, expert, 0)
    zero_stores(e_local - 1, wait)
    for e in range(max(e_local - 2, 0), e_local):
        dx_stores(e, e % 2, wait)
        dw_stores(e, e % 2, wait)


def grad_call(cnt, x_disp, ab, h, dy, w_gate, w_up):
    n_src, e_local, cap, dim = x_disp.shape
    ffn = w_gate.shape[2]
    most = n_src * cap
    hbm = pl.BlockSpec(memory_space=pl.ANY)
    dma = pltpu.SemaphoreType.DMA
    return pl.pallas_call(
        grad_kernel,
        out_shape=(jax.ShapeDtypeStruct(x_disp.shape, BF16), jax.ShapeDtypeStruct(w_gate.shape, BF16),
                   jax.ShapeDtypeStruct(w_up.shape, BF16), jax.ShapeDtypeStruct((e_local, ffn, dim), BF16)),
        in_specs=[pl.BlockSpec(memory_space=pltpu.SMEM)] + [hbm] * 6,
        out_specs=(hbm,) * 4,
        scratch_shapes=[
            pltpu.VMEM((2, most, dim), BF16), pltpu.VMEM((2, most, 2 * ffn), BF16),
            pltpu.VMEM((2, most, ffn), BF16), pltpu.VMEM((2, most, dim), BF16),
            pltpu.VMEM((2, dim, ffn), BF16), pltpu.VMEM((2, dim, ffn), BF16),
            pltpu.VMEM((2, most, dim), BF16),
            pltpu.VMEM((2, dim, ffn), BF16), pltpu.VMEM((2, dim, ffn), BF16), pltpu.VMEM((2, ffn, dim), BF16),
            pltpu.VMEM((cap, dim), BF16),
            dma((2, 4, n_src)), dma((2, 2)), dma((2, n_src)), dma((n_src,)), dma((2, 3)),
        ],
        compiler_params=pltpu.CompilerParams(vmem_limit_bytes=62 * 1024 * 1024),
        cost_estimate=pl.CostEstimate(flops=10 * n_src * e_local * cap * dim * ffn, bytes_accessed=64 * 2 ** 20, transcendentals=0),
        name='slot_gradients',
    )(cnt, x_disp, ab, h, dy, w_gate, w_up)


def solution(mesh):
    def local_step(x_disp, w_gate, w_up, w_down, d_out, slot_idx, expert_id, gate_wt):
        n_src, e_local = x_disp.shape[:2]
        tok = d_out.shape[0]
        h, ab, dy, gg, cnt = slot_call(x_disp, w_gate, w_up, w_down, d_out, slot_idx.T, expert_id.T, gate_wt.T)
        back = lax.all_to_all(gg.reshape(n_src, e_local, tok), 'ep', 0, 0, tiled=True).reshape(n_src * e_local, 1, tok)
        grad_x, grad_wg, grad_wu, grad_wd = grad_call(cnt, x_disp, ab, h, dy, w_gate, w_up)
        ids = lax.broadcasted_iota(jnp.int32, (n_src * e_local, 1, 1), 0)
        grad_gate = jnp.sum(jnp.where(expert_id.T[None] == ids, back, 0.0), axis=0).T
        return grad_x, grad_wg, grad_wu, grad_wd, grad_gate

    token_place = P(('dp', 'ep'), None)
    weight_place = P('ep', None, None)
    slot_place = P('dp', 'ep', None, None)
    grad_place = P(('dp', 'ep'), None, None)
    return jax.shard_map(local_step, mesh=mesh,
                         in_specs=(slot_place, weight_place, weight_place, weight_place, token_place, token_place, token_place, token_place),
                         out_specs=(slot_place, grad_place, grad_place, grad_place, token_place),
                         check_vma=False)
```

```python
import functools

import jax
import jax.numpy as jnp
from jax import lax
from jax.experimental import pallas as pl
from jax.experimental.pallas import tpu as pltpu
from jax.sharding import PartitionSpec as P

BF16 = jnp.bfloat16
F32 = jnp.float32
MESH = pl.DeviceIdType.MESH
NT = (((1,), (1,)), ((), ()))
TN = (((0,), (0,)), ((), ()))
PASS_AT = 5
TILE_M = 192


def slot_kernel(x_hbm, wg_hbm, wu_hbm, wd_hbm, d_hbm, slot_in, exp_in, gate_in,
                h_hbm, ab_hbm, dy_hbm, gg_out, cnt_ref,
                d_all, f1, f2, hid, m_slot, m_exp, m_gate, gg, gg_in, xb, wgb, wub, wdb, dbuf, abb,
                x_sem, w_sem, wd_sem, own_sem, h_sem, out_sem,
                link_send, link_recv, meta_send, meta_recv, gg_send, gg_recv):
    chips, cores = 4, 2
    n_dev = chips * cores
    e_local, cap = x_hbm.shape[1], x_hbm.shape[2]
    tok, dim, ffn = d_hbm.shape[0], d_hbm.shape[1], wg_hbm.shape[2]
    half = tok // 2
    quad = n_dev // 2
    blocks = 2 * e_local
    me = lax.axis_index('ep')
    chip, core = me // cores, me % cores
    right = lax.rem(chip + 1, chips)
    left = lax.rem(chip + chips - 1, chips)
    far = lax.rem(chip + 2, chips)
    to_right, to_left, to_sib = right * cores + core, left * cores + core, chip * cores + (1 - core)

    def x_copies(i, slot):
        return [pltpu.make_async_copy(x_hbm.at[(i % 2) * quad + k, i // 2], xb.at[slot, pl.ds(k * cap, cap)], x_sem.at[slot, k])
                for k in range(quad)]

    def w_copies(e, slot):
        return (pltpu.make_async_copy(wg_hbm.at[e], wgb.at[slot], w_sem.at[slot, 0]),
                pltpu.make_async_copy(wu_hbm.at[e], wub.at[slot], w_sem.at[slot, 1]))

    def h_copies(i):
        return [pltpu.make_async_copy(hid.at[i, pl.ds(k * cap, cap)], h_hbm.at[(i % 2) * quad + k, i // 2], h_sem.at[i, k])
                for k in range(quad)]

    def rows(h):
        return pl.ds(h * half, half)

    def link(src_ref, s, h, dst, n):
        return pltpu.make_async_remote_copy(src_ref=src_ref, dst_ref=d_all.at[s, rows(h)], send_sem=link_send.at[n],
                                            recv_sem=link_recv.at[s, h], device_id={'ep': dst}, device_id_type=MESH)

    def meta(k, other, s):
        src, dst = ((slot_in, m_slot), (exp_in, m_exp), (gate_in, m_gate))[k]
        return pltpu.make_async_remote_copy(src_ref=src, dst_ref=dst.at[s], send_sem=meta_send.at[k, other],
                                            recv_sem=meta_recv.at[k, s], device_id={'ep': other}, device_id_type=MESH)

    def gg_copy(other, s):
        return pltpu.make_async_remote_copy(src_ref=gg.at[other], dst_ref=gg_in.at[s], send_sem=gg_send.at[other],
                                            recv_sem=gg_recv.at[s], device_id={'ep': other}, device_id_type=MESH)

    def got(s, h):
        link(d_hbm.at[rows(h)], s, h, to_sib, 0).wait_recv()

    def peers(do):
        def step(k, carry):
            do(lax.rem(me + k, n_dev))
            return carry
        lax.fori_loop(1, n_dev, step, 0)

    barrier = pltpu.get_barrier_semaphore()
    peers(lambda other: pl.semaphore_signal(barrier, inc=1, device_id={'ep': other}, device_id_type=MESH))
    for c in x_copies(0, 0):
        c.start()
    for c in w_copies(0, 0):
        c.start()
    own_copy = pltpu.make_async_copy(d_hbm, d_all.at[me], own_sem)
    own_copy.start()
    wd_copy = pltpu.make_async_copy(wd_hbm, wdb, wd_sem)
    pl.semaphore_wait(barrier, n_dev - 1)

    own_links = [link(d_hbm.at[rows(h)], me, h, dst, n) for n, (dst, h) in enumerate(
        ((to_right, 0), (to_left, 1), (to_right, 1), (to_left, 0), (to_sib, 0), (to_sib, 1)))]
    for c in own_links:
        c.start()

    def send_meta(other):
        for a in range(3):
            meta(a, other, me).start()
    peers(send_meta)
    wd_copy.start()
    m_slot[me] = slot_in[...]
    m_exp[me] = exp_in[...]
    m_gate[me] = gate_in[...]

    l_src, r_src, f_src = left * cores + core, right * cores + core, far * cores + core
    pass_on = [link(d_all.at[l_src, rows(0)], l_src, 0, to_right, 6), link(d_all.at[r_src, rows(1)], r_src, 1, to_left, 7)]
    share = [link(d_all.at[s, rows(h)], s, h, to_sib, 8 + n) for n, (s, h) in enumerate(
        ((l_src, 0), (r_src, 1), (r_src, 0), (l_src, 1), (f_src, 0), (f_src, 1)))]

    def forward(i, carry):
        slot = i % 2
        e = i // 2

        @pl.when(i + 1 < blocks)
        def _():
            for c in x_copies(i + 1, 1 - slot):
                c.start()

        @pl.when(i % 2 == 0)
        def _():
            for c in w_copies(e, e % 2):
                c.wait()

            @pl.when(e + 1 < e_local)
            def _():
                for c in w_copies(e + 1, (e + 1) % 2):
                    c.start()

        for c in x_copies(i, slot):
            c.wait()

        @pl.when(i == PASS_AT)
        def _():
            got(l_src, 0)
            pass_on[0].start()
            got(r_src, 1)
            pass_on[1].start()
            share[0].start()
            share[1].start()

        for m in range(0, quad * cap, TILE_M):
            x = xb[slot, m:m + TILE_M]
            for n in range(0, ffn, 256):
                a = jnp.dot(x, wgb[e % 2, :, n:n + 256], preferred_element_type=F32)
                b = jnp.dot(x, wub[e % 2, :, n:n + 256], preferred_element_type=F32)
                sg = jax.nn.sigmoid(a)
                silu = a * sg
                f1[i, m:m + TILE_M, n:n + 256] = b * sg * (1.0 + a * (1.0 - sg))
                f2[i, m:m + TILE_M, n:n + 256] = silu
                hid[i, m:m + TILE_M, n:n + 256] = (silu * b).astype(BF16)
        for c in h_copies(i):
            c.start()
        return carry

    lax.fori_loop(0, blocks, forward, 0)

    own_copy.wait()
    wd_copy.wait()

    def got_meta(s):
        for a in range(3):
            meta(a, s, s).wait_recv()
    peers(got_meta)
    got(to_sib, 0)
    got(to_sib, 1)

    cap_ids = lax.broadcasted_iota(jnp.int32, (cap, tok), 0)

    def sources(g):
        near = ((g + 1) // 2) % 2
        c = (core + g // 2) % 2
        first = near * (left * cores + c) + (1 - near) * (lax.rem(chip + 2 * (g // 2), chips) * cores)
        second = near * (right * cores + c) + (1 - near) * (lax.rem(chip + 2 * (g // 2), chips) * cores + 1)
        return first, second

    def out_copies(j, slot):
        return [pltpu.make_async_copy(buf.at[slot, pl.ds((v * cores + k) * cap, cap)], dst.at[s, (j % 2) * 2 + v], out_sem.at[slot, a, v, k])
                for a, (buf, dst) in enumerate(((xb, dy_hbm), (abb, ab_hbm))) for v in range(2) for k, s in enumerate(sources(j // 2))]

    def backward(j, carry):
        slot = j % 2
        g = j // 2
        pair = sources(g)

        @pl.when(j == 2)
        def _():
            got(r_src, 0)
            share[2].start()
            got(l_src, 1)
            share[3].start()

        @pl.when(j == 4)
        def _():
            for s in (right * cores + 1 - core, left * cores + 1 - core):
                got(s, 0)
                got(s, 1)

        @pl.when(j == 6)
        def _():
            got(f_src, 0)
            share[4].start()
            got(f_src, 1)
            share[5].start()
            for h in range(2):
                got(far * cores + 1 - core, h)

        @pl.when(j >= 2)
        def _():
            for c in out_copies(j - 2, slot):
                c.wait()

        hits, gates = [], []
        for k, s in enumerate(pair):
            for v in range(2):
                e = (j % 2) * 2 + v
                slots = m_slot[s]
                match = (m_exp[s] == me * e_local + e) & (slots >= 0)
                at = jnp.sum(jnp.where(match, slots + 1, 0), axis=0, keepdims=True) - 1
                gate = jnp.sum(jnp.where(match, m_gate[s], 0.0), axis=0, keepdims=True)
                cnt_ref[s * e_local + e] = jnp.sum(jnp.where(match, 1, 0))
                hit = cap_ids == at
                hits.append(hit)
                gates.append(jnp.sum(jnp.where(hit, gate, 0.0), axis=1, keepdims=True))
        for k, s in enumerate(pair):
            pick = jnp.concatenate([jnp.where(hits[k * 2 + v], 1.0, 0.0).astype(BF16) for v in range(2)], axis=0)
            for n in range(0, dim, 256):
                d = jnp.dot(pick, d_all[s, :, n:n + 256], preferred_element_type=F32)
                for v in range(2):
                    at = (v * cores + k) * cap
                    dv = d[v * cap:(v + 1) * cap]
                    dbuf[at:at + cap, n:n + 256] = dv.astype(BF16)
                    xb[slot, at:at + cap, n:n + 256] = (dv * gates[k * 2 + v]).astype(BF16)
        for v in range(2):
            e = (j % 2) * 2 + v
            top = v * cores * cap
            dots = [jnp.zeros((cap, 1), F32) for _ in pair]
            for n in range(0, ffn, 256):
                u2 = lax.dot_general(dbuf[top:top + cores * cap], wdb[e, n:n + 256, :], NT, preferred_element_type=F32)
                for k, s in enumerate(pair):
                    i = e * 2 + s // quad
                    at = pl.ds(pl.multiple_of((s % quad) * cap, cap), cap)
                    u = u2[k * cap:(k + 1) * cap]
                    dots[k] = dots[k] + jnp.sum(u * hid[i, at, n:n + 256].astype(F32), axis=1, keepdims=True)
                    dh = (u * gates[k * 2 + v]).astype(BF16).astype(F32)
                    to = pl.ds(top + k * cap, cap)
                    abb[slot, to, n:n + 256] = (dh * f1[i, at, n:n + 256]).astype(BF16)
                    abb[slot, to, ffn + n:ffn + n + 256] = (dh * f2[i, at, n:n + 256]).astype(BF16)
            for k, s in enumerate(pair):
                gg[s, e] = jnp.sum(jnp.where(hits[k * 2 + v], dots[k], 0.0), axis=0, keepdims=True)
        for c in out_copies(j, slot):
            c.start()

        @pl.when((j % 2 == 1) & (j > 1))
        def _():
            for s in pair:
                gg_copy(s, me).start()

        @pl.when(j == 1)
        def _():
            gg_copy(to_sib, me).start()
        return carry

    lax.fori_loop(0, blocks, backward, 0)
    for j in (blocks - 2, blocks - 1):
        for c in out_copies(j, j % 2):
            c.wait()

    def h_done(i, carry):
        for c in h_copies(i):
            c.wait()
        return carry
    lax.fori_loop(0, blocks, h_done, 0)

    def sent(other):
        for a in range(3):
            meta(a, other, me).wait_send()
        gg_copy(other, me).wait_send()
    peers(sent)
    for c in own_links + pass_on + share:
        c.wait_send()
    gg_in[me] = gg[me]
    peers(lambda s: gg_copy(s, s).wait_recv())
    gg_out[...] = gg_in[...]


def slot_call(x_disp, w_gate, w_up, w_down, d_out, slot_t, exp_t, gate_t):
    n_src, e_local, cap, dim = x_disp.shape
    ffn = w_gate.shape[2]
    tok, top_k = d_out.shape[0], slot_t.shape[0]
    blocks, quad = 2 * e_local, n_src // 2
    hbm = pl.BlockSpec(memory_space=pl.ANY)
    vmem = pl.BlockSpec(memory_space=pltpu.VMEM)
    smem = pl.BlockSpec(memory_space=pltpu.SMEM)
    dma = pltpu.SemaphoreType.DMA
    return pl.pallas_call(
        slot_kernel,
        out_shape=(jax.ShapeDtypeStruct((n_src, e_local, cap, ffn), BF16),
                   jax.ShapeDtypeStruct((n_src, e_local, cap, 2 * ffn), BF16),
                   jax.ShapeDtypeStruct((n_src, e_local, cap, dim), BF16),
                   jax.ShapeDtypeStruct((n_src, e_local, 1, tok), F32),
                   jax.ShapeDtypeStruct((n_src * e_local,), jnp.int32)),
        in_specs=[hbm] * 5 + [vmem] * 3,
        out_specs=(hbm, hbm, hbm, vmem, smem),
        scratch_shapes=[
            pltpu.VMEM((n_src, tok, dim), BF16),
            pltpu.VMEM((blocks, quad * cap, ffn), F32), pltpu.VMEM((blocks, quad * cap, ffn), F32),
            pltpu.VMEM((blocks, quad * cap, ffn), BF16),
            pltpu.VMEM((n_src, top_k, tok), jnp.int32), pltpu.VMEM((n_src, top_k, tok), jnp.int32), pltpu.VMEM((n_src, top_k, tok), F32),
            pltpu.VMEM((n_src, e_local, 1, tok), F32), pltpu.VMEM((n_src, e_local, 1, tok), F32),
            pltpu.VMEM((2, quad * cap, dim), BF16),
            pltpu.VMEM((2, dim, ffn), BF16), pltpu.VMEM((2, dim, ffn), BF16), pltpu.VMEM((e_local, ffn, dim), BF16),
            pltpu.VMEM((quad * cap, dim), BF16), pltpu.VMEM((2, quad * cap, 2 * ffn), BF16),
            dma((2, quad)), dma((2, 2)), dma, dma, dma((blocks, quad)), dma((2, 2, 2, 2)),
            dma((14,)), dma((n_src, 2)), dma((3, n_src)), dma((3, n_src)), dma((n_src,)), dma((n_src,)),
        ],
        compiler_params=pltpu.CompilerParams(collective_id=0, has_side_effects=True, vmem_limit_bytes=62 * 1024 * 1024),
        cost_estimate=pl.CostEstimate(flops=8 * n_src * e_local * cap * dim * ffn, bytes_accessed=64 * 2 ** 20, transcendentals=0),
        name='slot_cotangents',
    )(x_disp, w_gate, w_up, w_down, d_out, slot_t, exp_t, gate_t)


def grad_kernel(cnt, x_hbm, ab_hbm, h_hbm, dy_hbm, wg_hbm, wu_hbm, gg, exp_in,
                dx_hbm, dwg_hbm, dwu_hbm, dwd_hbm, gate_out,
                xb, abb, hb, dyb, wgb, wub, dxb, dwgb, dwub, dwdb, zeros,
                in_sem, w_sem, dx_sem, z_sem, dw_sem):
    n_src, e_local, cap, dim = x_hbm.shape
    ffn = wg_hbm.shape[2]
    step, grain = 256, 16
    pairs = ((x_hbm, xb), (ab_hbm, abb), (h_hbm, hb), (dy_hbm, dyb))

    def spans(e):
        out, start = [], jnp.int32(0)
        for s in range(n_src):
            n = (cnt[s * e_local + e] + (grain - 1)) // grain * grain
            out.append((pl.multiple_of(start, grain), pl.multiple_of(n, grain)))
            start = start + n
        return out, pl.multiple_of(start, grain)

    def loads(e, slot, do):
        for s, (start, n) in enumerate(spans(e)[0]):
            @pl.when(n > 0)
            def _():
                for j, (src, dst) in enumerate(pairs):
                    do(pltpu.make_async_copy(src.at[s, e, pl.ds(0, n)], dst.at[slot, pl.ds(start, n)], in_sem.at[slot, j, s]))
        do(pltpu.make_async_copy(wg_hbm.at[e], wgb.at[slot], w_sem.at[slot, 0]))
        do(pltpu.make_async_copy(wu_hbm.at[e], wub.at[slot], w_sem.at[slot, 1]))

    def dx_stores(e, slot, do):
        for s, (start, n) in enumerate(spans(e)[0]):
            @pl.when(n > 0)
            def _():
                do(pltpu.make_async_copy(dxb.at[slot, pl.ds(start, n)], dx_hbm.at[s, e, pl.ds(0, n)], dx_sem.at[slot, s]))

    def zero_stores(e, do):
        for s, (_, n) in enumerate(spans(e)[0]):
            rest = pl.multiple_of(cap - n, grain)

            @pl.when(rest > 0)
            def _():
                do(pltpu.make_async_copy(zeros.at[pl.ds(0, rest)], dx_hbm.at[s, e, pl.ds(n, rest)], z_sem.at[s]))

    def dw_stores(e, slot, do):
        for j, (src, dst) in enumerate(((dwgb, dwg_hbm), (dwub, dwu_hbm), (dwdb, dwd_hbm))):
            do(pltpu.make_async_copy(src.at[slot], dst.at[e], dw_sem.at[slot, j]))

    start = lambda c: c.start()
    wait = lambda c: c.wait()

    loads(0, 0, start)
    zeros[...] = jnp.zeros_like(zeros)
    ids = exp_in[...]
    gate_out[...] = sum(jnp.where(ids == s * e_local + e, gg[s, e], 0.0) for s in range(n_src) for e in range(e_local))

    def expert(e, carry):
        slot = e % 2

        @pl.when(e + 1 < e_local)
        def _():
            loads(e + 1, 1 - slot, start)

        @pl.when(e > 0)
        def _():
            zero_stores(e - 1, wait)
        zero_stores(e, start)
        loads(e, slot, wait)

        @pl.when(e >= 2)
        def _():
            dx_stores(e - 2, slot, wait)
            dw_stores(e - 2, slot, wait)

        total = spans(e)[1]
        count = jnp.maximum((total + (step - 1)) // step, 1)

        def clear(j, c):
            at = pl.ds(pl.multiple_of(total + j * grain, grain), grain)
            for buf in (xb, abb, hb, dyb):
                buf[slot, at, :] = jnp.zeros((grain, buf.shape[2]), BF16)
            return c
        lax.fori_loop(0, (count * step - total) // grain, clear, 0)

        for k in range(1, n_src * cap // step + 1):
            rows = k * step

            @pl.when(count == k)
            def _():
                def tiles(t, c):
                    for r in range(2):
                        at = pl.ds(pl.multiple_of((t * 2 + r) * 256, 256), 256)
                        dxb[slot, :rows, at] = (
                            lax.dot_general(abb[slot, :rows, :ffn], wgb[slot, at, :], NT, preferred_element_type=F32)
                            + lax.dot_general(abb[slot, :rows, ffn:], wub[slot, at, :], NT, preferred_element_type=F32)).astype(BF16)
                        up = lax.dot_general(xb[slot, :rows, at], abb[slot, :rows, :], TN, preferred_element_type=F32).astype(BF16)
                        dwgb[slot, at, :] = up[:, :ffn]
                        dwub[slot, at, :] = up[:, ffn:]
                    at = pl.ds(pl.multiple_of(t * 256, 256), 256)
                    dwdb[slot, at, :] = lax.dot_general(hb[slot, :rows, at], dyb[slot, :rows, :], TN, preferred_element_type=F32).astype(BF16)
                    return c
                lax.fori_loop(0, ffn // 256, tiles, 0)

        dx_stores(e, slot, start)
        dw_stores(e, slot, start)
        return carry

    lax.fori_loop(0, e_local, expert, 0)
    zero_stores(e_local - 1, wait)
    for e in range(max(e_local - 2, 0), e_local):
        dx_stores(e, e % 2, wait)
        dw_stores(e, e % 2, wait)


def grad_call(cnt, x_disp, ab, h, dy, w_gate, w_up, gg, exp_t):
    n_src, e_local, cap, dim = x_disp.shape
    ffn = w_gate.shape[2]
    most = n_src * cap
    hbm = pl.BlockSpec(memory_space=pl.ANY)
    vmem = pl.BlockSpec(memory_space=pltpu.VMEM)
    dma = pltpu.SemaphoreType.DMA
    return pl.pallas_call(
        grad_kernel,
        out_shape=(jax.ShapeDtypeStruct(x_disp.shape, BF16), jax.ShapeDtypeStruct(w_gate.shape, BF16),
                   jax.ShapeDtypeStruct(w_up.shape, BF16), jax.ShapeDtypeStruct((e_local, ffn, dim), BF16), jax.ShapeDtypeStruct(exp_t.shape, F32)),
        in_specs=[pl.BlockSpec(memory_space=pltpu.SMEM)] + [hbm] * 6 + [vmem] * 2,
        out_specs=(hbm,) * 4 + (vmem,),
        scratch_shapes=[
            pltpu.VMEM((2, most, dim), BF16), pltpu.VMEM((2, most, 2 * ffn), BF16),
            pltpu.VMEM((2, most, ffn), BF16), pltpu.VMEM((2, most, dim), BF16),
            pltpu.VMEM((2, dim, ffn), BF16), pltpu.VMEM((2, dim, ffn), BF16),
            pltpu.VMEM((2, most, dim), BF16),
            pltpu.VMEM((2, dim, ffn), BF16), pltpu.VMEM((2, dim, ffn), BF16), pltpu.VMEM((2, ffn, dim), BF16),
            pltpu.VMEM((cap, dim), BF16),
            dma((2, 4, n_src)), dma((2, 2)), dma((2, n_src)), dma((n_src,)), dma((2, 3)),
        ],
        compiler_params=pltpu.CompilerParams(vmem_limit_bytes=62 * 1024 * 1024),
        cost_estimate=pl.CostEstimate(flops=10 * n_src * e_local * cap * dim * ffn, bytes_accessed=64 * 2 ** 20, transcendentals=0),
        name='slot_gradients',
    )(cnt, x_disp, ab, h, dy, w_gate, w_up, gg, exp_t)


def solution(mesh):
    def local_step(x_disp, w_gate, w_up, w_down, d_out, slot_idx, expert_id, gate_wt):
        exp_t = expert_id.T
        h, ab, dy, gg, cnt = slot_call(x_disp, w_gate, w_up, w_down, d_out, slot_idx.T, exp_t, gate_wt.T)
        grad_x, grad_wg, grad_wu, grad_wd, gate_t = grad_call(cnt, x_disp, ab, h, dy, w_gate, w_up, gg, exp_t)
        return grad_x, grad_wg, grad_wu, grad_wd, gate_t.T

    token_place = P(('dp', 'ep'), None)
    weight_place = P('ep', None, None)
    slot_place = P('dp', 'ep', None, None)
    grad_place = P(('dp', 'ep'), None, None)
    return jax.shard_map(local_step, mesh=mesh,
                         in_specs=(slot_place, weight_place, weight_place, weight_place, token_place, token_place, token_place, token_place),
                         out_specs=(slot_place, grad_place, grad_place, grad_place, token_place),
                         check_vma=False)
```

```python
import functools

import jax
import jax.numpy as jnp
from jax import lax
from jax.experimental import pallas as pl
from jax.experimental.pallas import tpu as pltpu
from jax.sharding import PartitionSpec as P

BF16 = jnp.bfloat16
F32 = jnp.float32
MESH = pl.DeviceIdType.MESH
NT = (((1,), (1,)), ((), ()))
TN = (((0,), (0,)), ((), ()))
PASS_AT = 6
FAR_AT = 5
TILE_M = 192


def slot_kernel(x_hbm, wg_hbm, wu_hbm, wd_hbm, d_hbm, slot_in, exp_in, gate_in,
                h_hbm, ab_hbm, dy_hbm, gg_out, cnt_ref,
                d_all, f1, f2, hid, m_all, gg, gg_in, xb, wgb, wub, wdb, dbuf, abb,
                x_sem, w_sem, wd_sem, own_sem, h_sem, out_sem,
                link_send, link_recv, meta_send, meta_recv, gg_send, gg_recv):
    chips, cores = 4, 2
    n_dev = chips * cores
    e_local, cap = x_hbm.shape[1], x_hbm.shape[2]
    tok, dim, ffn = d_hbm.shape[0], d_hbm.shape[1], wg_hbm.shape[2]
    top_k = slot_in.shape[0]
    half = tok // 2
    quad = n_dev // 2
    blocks = 2 * e_local
    me = lax.axis_index('ep')
    chip, core = me // cores, me % cores
    right = lax.rem(chip + 1, chips)
    left = lax.rem(chip + chips - 1, chips)
    far = lax.rem(chip + 2, chips)
    to_right, to_left, to_sib = right * cores + core, left * cores + core, chip * cores + (1 - core)

    def x_copies(i, slot):
        return [pltpu.make_async_copy(x_hbm.at[(i % 2) * quad + k, i // 2], xb.at[slot, pl.ds(k * cap, cap)], x_sem.at[slot, k])
                for k in range(quad)]

    def w_copies(e, slot):
        return (pltpu.make_async_copy(wg_hbm.at[e], wgb.at[slot], w_sem.at[slot, 0]),
                pltpu.make_async_copy(wu_hbm.at[e], wub.at[slot], w_sem.at[slot, 1]))

    def h_copies(i):
        return [pltpu.make_async_copy(hid.at[i, pl.ds(k * cap, cap)], h_hbm.at[(i % 2) * quad + k, i // 2], h_sem.at[i, k])
                for k in range(quad)]

    def rows(h):
        return pl.ds(h * half, half)

    def link(src_ref, s, h, dst, n):
        return pltpu.make_async_remote_copy(src_ref=src_ref, dst_ref=d_all.at[s, rows(h)], send_sem=link_send.at[n],
                                            recv_sem=link_recv.at[s, h], device_id={'ep': dst}, device_id_type=MESH)

    def meta(s, dst, n):
        return pltpu.make_async_remote_copy(src_ref=m_all.at[s], dst_ref=m_all.at[s], send_sem=meta_send.at[n],
                                            recv_sem=meta_recv.at[s], device_id={'ep': dst}, device_id_type=MESH)

    def gg_copy(other, s):
        return pltpu.make_async_remote_copy(src_ref=gg.at[other], dst_ref=gg_in.at[s], send_sem=gg_send.at[other],
                                            recv_sem=gg_recv.at[s], device_id={'ep': other}, device_id_type=MESH)

    def got(s, h):
        link(d_hbm.at[rows(h)], s, h, to_sib, 0).wait_recv()

    def peers(do):
        def step(k, carry):
            do(lax.rem(me + k, n_dev))
            return carry
        lax.fori_loop(1, n_dev, step, 0)

    m_all[me, :top_k] = slot_in[...].astype(F32)
    m_all[me, top_k:2 * top_k] = exp_in[...].astype(F32)
    m_all[me, 2 * top_k:] = gate_in[...]
    barrier = pltpu.get_barrier_semaphore()
    peers(lambda other: pl.semaphore_signal(barrier, inc=1, device_id={'ep': other}, device_id_type=MESH))
    for c in x_copies(0, 0):
        c.start()
    for c in w_copies(0, 0):
        c.start()
    own_copy = pltpu.make_async_copy(d_hbm, d_all.at[me], own_sem)
    own_copy.start()
    wd_copy = pltpu.make_async_copy(wd_hbm, wdb, wd_sem)
    pl.semaphore_wait(barrier, n_dev - 1)

    own_links = [link(d_hbm.at[rows(h)], me, h, dst, n) for n, (dst, h) in enumerate(
        ((to_right, 0), (to_left, 1), (to_right, 1), (to_left, 0), (to_sib, 0), (to_sib, 1)))]
    to_far = far * cores + core
    own_meta = [meta(me, dst, n) for n, dst in enumerate((to_right, to_left, to_far, to_sib))]
    for c in own_meta + own_links:
        c.start()
    wd_copy.start()

    l_src, r_src, f_src = left * cores + core, right * cores + core, far * cores + core
    pass_on = [link(d_all.at[l_src, rows(0)], l_src, 0, to_right, 6), link(d_all.at[r_src, rows(1)], r_src, 1, to_left, 7)]
    share = [link(d_all.at[s, rows(h)], s, h, to_sib, 8 + n) for n, (s, h) in enumerate(
        ((l_src, 0), (r_src, 1), (r_src, 0), (l_src, 1), (f_src, 0), (f_src, 1)))]

    share_meta = [meta(s, to_sib, 4 + n) for n, s in enumerate((l_src, r_src, f_src))]

    def forward(i, carry):
        slot = i % 2
        e = i // 2

        @pl.when(i + 1 < blocks)
        def _():
            for c in x_copies(i + 1, 1 - slot):
                c.start()

        @pl.when(i % 2 == 0)
        def _():
            for c in w_copies(e, e % 2):
                c.wait()

            @pl.when(e + 1 < e_local)
            def _():
                for c in w_copies(e + 1, (e + 1) % 2):
                    c.start()

        for c in x_copies(i, slot):
            c.wait()

        @pl.when(i == 3)
        def _():
            for n, s in enumerate((l_src, r_src, f_src)):
                meta(s, to_sib, 0).wait_recv()
                share_meta[n].start()

        @pl.when(i == PASS_AT)
        def _():
            got(l_src, 0)
            pass_on[0].start()
            got(r_src, 1)
            pass_on[1].start()

        for m in range(0, quad * cap, TILE_M):
            x = xb[slot, m:m + TILE_M]
            for n in range(0, ffn, 256):
                a = jnp.dot(x, wgb[e % 2, :, n:n + 256], preferred_element_type=F32)
                b = jnp.dot(x, wub[e % 2, :, n:n + 256], preferred_element_type=F32)
                sg = jax.nn.sigmoid(a)
                silu = a * sg
                f1[i, m:m + TILE_M, n:n + 256] = b * sg * (1.0 + a * (1.0 - sg))
                f2[i, m:m + TILE_M, n:n + 256] = silu
                hid[i, m:m + TILE_M, n:n + 256] = (silu * b).astype(BF16)
        for c in h_copies(i):
            c.start()
        return carry

    lax.fori_loop(0, blocks, forward, 0)

    own_copy.wait()
    wd_copy.wait()

    for s in (to_sib, left * cores + 1 - core, right * cores + 1 - core, far * cores + 1 - core):
        meta(s, to_sib, 0).wait_recv()
    got(to_sib, 0)
    got(to_sib, 1)

    cap_ids = lax.broadcasted_iota(jnp.int32, (cap, tok), 0).astype(F32)

    def sources(g):
        near = ((g + 1) // 2) % 2
        c = (core + g // 2) % 2
        first = near * (left * cores + c) + (1 - near) * (lax.rem(chip + 2 * (g // 2), chips) * cores)
        second = near * (right * cores + c) + (1 - near) * (lax.rem(chip + 2 * (g // 2), chips) * cores + 1)
        return first, second

    def out_copies(j, slot):
        return [pltpu.make_async_copy(buf.at[slot, pl.ds((v * cores + k) * cap, cap)], dst.at[s, (j % 2) * 2 + v], out_sem.at[slot, a, v, k])
                for a, (buf, dst) in enumerate(((xb, dy_hbm), (abb, ab_hbm))) for v in range(2) for k, s in enumerate(sources(j // 2))]

    def backward(j, carry):
        slot = j % 2
        g = j // 2
        pair = sources(g)

        @pl.when(j == 2)
        def _():
            got(r_src, 0)
            got(l_src, 1)
            for c in share[:4]:
                c.start()

        @pl.when(j == 4)
        def _():
            for s in (right * cores + 1 - core, left * cores + 1 - core):
                got(s, 0)
                got(s, 1)

        @pl.when(j == FAR_AT)
        def _():
            got(f_src, 0)
            share[4].start()
            got(f_src, 1)
            share[5].start()

        @pl.when(j == 6)
        def _():
            for h in range(2):
                got(far * cores + 1 - core, h)

        @pl.when(j >= 2)
        def _():
            for c in out_copies(j - 2, slot):
                c.wait()

        hits, gates = [], []
        for k, s in enumerate(pair):
            for v in range(2):
                e = (j % 2) * 2 + v
                slots = m_all[s, :top_k]
                match = (m_all[s, top_k:2 * top_k] == (me * e_local + e).astype(F32)) & (slots >= 0.0)
                at = jnp.sum(jnp.where(match, slots + 1.0, 0.0), axis=0, keepdims=True) - 1.0
                gate = jnp.sum(jnp.where(match, m_all[s, 2 * top_k:], 0.0), axis=0, keepdims=True)
                cnt_ref[s * e_local + e] = jnp.sum(jnp.where(match, 1, 0))
                hit = cap_ids == at
                hits.append(hit)
                gates.append(jnp.sum(jnp.where(hit, gate, 0.0), axis=1, keepdims=True))
        for k, s in enumerate(pair):
            pick = jnp.concatenate([jnp.where(hits[k * 2 + v], 1.0, 0.0).astype(BF16) for v in range(2)], axis=0)
            for n in range(0, dim, 256):
                d = jnp.dot(pick, d_all[s, :, n:n + 256], preferred_element_type=F32)
                for v in range(2):
                    at = (v * cores + k) * cap
                    dv = d[v * cap:(v + 1) * cap]
                    dbuf[at:at + cap, n:n + 256] = dv.astype(BF16)
                    xb[slot, at:at + cap, n:n + 256] = (dv * gates[k * 2 + v]).astype(BF16)
        for v in range(2):
            e = (j % 2) * 2 + v
            top = v * cores * cap
            dots = [jnp.zeros((cap, 1), F32) for _ in pair]
            for n in range(0, ffn, 256):
                u2 = lax.dot_general(dbuf[top:top + cores * cap], wdb[e, n:n + 256, :], NT, preferred_element_type=F32)
                for k, s in enumerate(pair):
                    i = e * 2 + s // quad
                    at = pl.ds(pl.multiple_of((s % quad) * cap, cap), cap)
                    u = u2[k * cap:(k + 1) * cap]
                    dots[k] = dots[k] + jnp.sum(u * hid[i, at, n:n + 256].astype(F32), axis=1, keepdims=True)
                    dh = (u * gates[k * 2 + v]).astype(BF16).astype(F32)
                    to = pl.ds(top + k * cap, cap)
                    abb[slot, to, n:n + 256] = (dh * f1[i, at, n:n + 256]).astype(BF16)
                    abb[slot, to, ffn + n:ffn + n + 256] = (dh * f2[i, at, n:n + 256]).astype(BF16)
            for k, s in enumerate(pair):
                gg[s, e] = jnp.sum(jnp.where(hits[k * 2 + v], dots[k], 0.0), axis=0, keepdims=True)
        for c in out_copies(j, slot):
            c.start()

        @pl.when((j % 2 == 1) & (j > 1))
        def _():
            for s in pair:
                gg_copy(s, me).start()

        @pl.when(j == 1)
        def _():
            gg_copy(to_sib, me).start()
        return carry

    lax.fori_loop(0, blocks, backward, 0)
    for j in (blocks - 2, blocks - 1):
        for c in out_copies(j, j % 2):
            c.wait()

    def h_done(i, carry):
        for c in h_copies(i):
            c.wait()
        return carry
    lax.fori_loop(0, blocks, h_done, 0)

    def sent(other):
        gg_copy(other, me).wait_send()
    peers(sent)
    for c in own_meta + share_meta + own_links + pass_on + share:
        c.wait_send()
    gg_in[me] = gg[me]
    peers(lambda s: gg_copy(s, s).wait_recv())
    gg_out[...] = gg_in[...]


def slot_call(x_disp, w_gate, w_up, w_down, d_out, slot_t, exp_t, gate_t):
    n_src, e_local, cap, dim = x_disp.shape
    ffn = w_gate.shape[2]
    tok, top_k = d_out.shape[0], slot_t.shape[0]
    blocks, quad = 2 * e_local, n_src // 2
    hbm = pl.BlockSpec(memory_space=pl.ANY)
    vmem = pl.BlockSpec(memory_space=pltpu.VMEM)
    smem = pl.BlockSpec(memory_space=pltpu.SMEM)
    dma = pltpu.SemaphoreType.DMA
    return pl.pallas_call(
        slot_kernel,
        out_shape=(jax.ShapeDtypeStruct((n_src, e_local, cap, ffn), BF16),
                   jax.ShapeDtypeStruct((n_src, e_local, cap, 2 * ffn), BF16),
                   jax.ShapeDtypeStruct((n_src, e_local, cap, dim), BF16),
                   jax.ShapeDtypeStruct((n_src, e_local, 1, tok), F32),
                   jax.ShapeDtypeStruct((n_src * e_local,), jnp.int32)),
        in_specs=[hbm] * 5 + [vmem] * 3,
        out_specs=(hbm, hbm, hbm, vmem, smem),
        scratch_shapes=[
            pltpu.VMEM((n_src, tok, dim), BF16),
            pltpu.VMEM((blocks, quad * cap, ffn), F32), pltpu.VMEM((blocks, quad * cap, ffn), F32),
            pltpu.VMEM((blocks, quad * cap, ffn), BF16),
            pltpu.VMEM((n_src, 3 * top_k, tok), F32),
            pltpu.VMEM((n_src, e_local, 1, tok), F32), pltpu.VMEM((n_src, e_local, 1, tok), F32),
            pltpu.VMEM((2, quad * cap, dim), BF16),
            pltpu.VMEM((2, dim, ffn), BF16), pltpu.VMEM((2, dim, ffn), BF16), pltpu.VMEM((e_local, ffn, dim), BF16),
            pltpu.VMEM((quad * cap, dim), BF16), pltpu.VMEM((2, quad * cap, 2 * ffn), BF16),
            dma((2, quad)), dma((2, 2)), dma, dma, dma((blocks, quad)), dma((2, 2, 2, 2)),
            dma((14,)), dma((n_src, 2)), dma((7,)), dma((n_src,)), dma((n_src,)), dma((n_src,)),
        ],
        compiler_params=pltpu.CompilerParams(collective_id=0, has_side_effects=True, vmem_limit_bytes=62 * 1024 * 1024),
        cost_estimate=pl.CostEstimate(flops=8 * n_src * e_local * cap * dim * ffn, bytes_accessed=64 * 2 ** 20, transcendentals=0),
        name='slot_cotangents',
    )(x_disp, w_gate, w_up, w_down, d_out, slot_t, exp_t, gate_t)


def grad_kernel(cnt, x_hbm, ab_hbm, h_hbm, dy_hbm, wg_hbm, wu_hbm, gg, exp_in,
                dx_hbm, dwg_hbm, dwu_hbm, dwd_hbm, gate_out,
                xb, abb, hb, dyb, wgb, wub, dxb, dwgb, dwub, dwdb, zeros,
                in_sem, w_sem, dx_sem, z_sem, dw_sem):
    n_src, e_local, cap, dim = x_hbm.shape
    ffn = wg_hbm.shape[2]
    step, grain = 256, 16
    pairs = ((x_hbm, xb), (ab_hbm, abb), (h_hbm, hb), (dy_hbm, dyb))

    def spans(e):
        out, start = [], jnp.int32(0)
        for s in range(n_src):
            n = (cnt[s * e_local + e] + (grain - 1)) // grain * grain
            out.append((pl.multiple_of(start, grain), pl.multiple_of(n, grain)))
            start = start + n
        return out, pl.multiple_of(start, grain)

    def loads(e, slot, do):
        for s, (start, n) in enumerate(spans(e)[0]):
            @pl.when(n > 0)
            def _():
                for j, (src, dst) in enumerate(pairs):
                    do(pltpu.make_async_copy(src.at[s, e, pl.ds(0, n)], dst.at[slot, pl.ds(start, n)], in_sem.at[slot, j, s]))
        do(pltpu.make_async_copy(wg_hbm.at[e], wgb.at[slot], w_sem.at[slot, 0]))
        do(pltpu.make_async_copy(wu_hbm.at[e], wub.at[slot], w_sem.at[slot, 1]))

    def dx_stores(e, slot, do):
        for s, (start, n) in enumerate(spans(e)[0]):
            @pl.when(n > 0)
            def _():
                do(pltpu.make_async_copy(dxb.at[slot, pl.ds(start, n)], dx_hbm.at[s, e, pl.ds(0, n)], dx_sem.at[slot, s]))

    def zero_stores(e, do):
        for s, (_, n) in enumerate(spans(e)[0]):
            rest = pl.multiple_of(cap - n, grain)

            @pl.when(rest > 0)
            def _():
                do(pltpu.make_async_copy(zeros.at[pl.ds(0, rest)], dx_hbm.at[s, e, pl.ds(n, rest)], z_sem.at[s]))

    def dw_stores(e, slot, do):
        for j, (src, dst) in enumerate(((dwgb, dwg_hbm), (dwub, dwu_hbm), (dwdb, dwd_hbm))):
            do(pltpu.make_async_copy(src.at[slot], dst.at[e], dw_sem.at[slot, j]))

    start = lambda c: c.start()
    wait = lambda c: c.wait()

    loads(0, 0, start)
    zeros[...] = jnp.zeros_like(zeros)
    ids = exp_in[...]
    gate_out[...] = sum(jnp.where(ids == s * e_local + e, gg[s, e], 0.0) for s in range(n_src) for e in range(e_local))

    def expert(e, carry):
        slot = e % 2

        @pl.when(e + 1 < e_local)
        def _():
            loads(e + 1, 1 - slot, start)

        @pl.when(e > 0)
        def _():
            zero_stores(e - 1, wait)
        zero_stores(e, start)
        loads(e, slot, wait)

        @pl.when(e >= 2)
        def _():
            dx_stores(e - 2, slot, wait)
            dw_stores(e - 2, slot, wait)

        total = spans(e)[1]
        count = jnp.maximum((total + (step - 1)) // step, 1)

        def clear(j, c):
            at = pl.ds(pl.multiple_of(total + j * grain, grain), grain)
            for buf in (xb, abb, hb, dyb):
                buf[slot, at, :] = jnp.zeros((grain, buf.shape[2]), BF16)
            return c
        lax.fori_loop(0, (count * step - total) // grain, clear, 0)

        for k in range(1, n_src * cap // step + 1):
            rows = k * step

            @pl.when(count == k)
            def _():
                def tiles(t, c):
                    for r in range(2):
                        at = pl.ds(pl.multiple_of((t * 2 + r) * 256, 256), 256)
                        dxb[slot, :rows, at] = (
                            lax.dot_general(abb[slot, :rows, :ffn], wgb[slot, at, :], NT, preferred_element_type=F32)
                            + lax.dot_general(abb[slot, :rows, ffn:], wub[slot, at, :], NT, preferred_element_type=F32)).astype(BF16)
                        up = lax.dot_general(xb[slot, :rows, at], abb[slot, :rows, :], TN, preferred_element_type=F32).astype(BF16)
                        dwgb[slot, at, :] = up[:, :ffn]
                        dwub[slot, at, :] = up[:, ffn:]
                    at = pl.ds(pl.multiple_of(t * 256, 256), 256)
                    dwdb[slot, at, :] = lax.dot_general(hb[slot, :rows, at], dyb[slot, :rows, :], TN, preferred_element_type=F32).astype(BF16)
                    return c
                lax.fori_loop(0, ffn // 256, tiles, 0)

        dx_stores(e, slot, start)
        dw_stores(e, slot, start)
        return carry

    lax.fori_loop(0, e_local, expert, 0)
    zero_stores(e_local - 1, wait)
    for e in range(max(e_local - 2, 0), e_local):
        dx_stores(e, e % 2, wait)
        dw_stores(e, e % 2, wait)


def grad_call(cnt, x_disp, ab, h, dy, w_gate, w_up, gg, exp_t):
    n_src, e_local, cap, dim = x_disp.shape
    ffn = w_gate.shape[2]
    most = n_src * cap
    hbm = pl.BlockSpec(memory_space=pl.ANY)
    vmem = pl.BlockSpec(memory_space=pltpu.VMEM)
    dma = pltpu.SemaphoreType.DMA
    return pl.pallas_call(
        grad_kernel,
        out_shape=(jax.ShapeDtypeStruct(x_disp.shape, BF16), jax.ShapeDtypeStruct(w_gate.shape, BF16),
                   jax.ShapeDtypeStruct(w_up.shape, BF16), jax.ShapeDtypeStruct((e_local, ffn, dim), BF16), jax.ShapeDtypeStruct(exp_t.shape, F32)),
        in_specs=[pl.BlockSpec(memory_space=pltpu.SMEM)] + [hbm] * 6 + [vmem] * 2,
        out_specs=(hbm,) * 4 + (vmem,),
        scratch_shapes=[
            pltpu.VMEM((2, most, dim), BF16), pltpu.VMEM((2, most, 2 * ffn), BF16),
            pltpu.VMEM((2, most, ffn), BF16), pltpu.VMEM((2, most, dim), BF16),
            pltpu.VMEM((2, dim, ffn), BF16), pltpu.VMEM((2, dim, ffn), BF16),
            pltpu.VMEM((2, most, dim), BF16),
            pltpu.VMEM((2, dim, ffn), BF16), pltpu.VMEM((2, dim, ffn), BF16), pltpu.VMEM((2, ffn, dim), BF16),
            pltpu.VMEM((cap, dim), BF16),
            dma((2, 4, n_src)), dma((2, 2)), dma((2, n_src)), dma((n_src,)), dma((2, 3)),
        ],
        compiler_params=pltpu.CompilerParams(vmem_limit_bytes=62 * 1024 * 1024),
        cost_estimate=pl.CostEstimate(flops=10 * n_src * e_local * cap * dim * ffn, bytes_accessed=64 * 2 ** 20, transcendentals=0),
        name='slot_gradients',
    )(cnt, x_disp, ab, h, dy, w_gate, w_up, gg, exp_t)


def solution(mesh):
    def local_step(x_disp, w_gate, w_up, w_down, d_out, slot_idx, expert_id, gate_wt):
        exp_t = expert_id.T
        h, ab, dy, gg, cnt = slot_call(x_disp, w_gate, w_up, w_down, d_out, slot_idx.T, exp_t, gate_wt.T)
        grad_x, grad_wg, grad_wu, grad_wd, gate_t = grad_call(cnt, x_disp, ab, h, dy, w_gate, w_up, gg, exp_t)
        return grad_x, grad_wg, grad_wu, grad_wd, gate_t.T

    token_place = P(('dp', 'ep'), None)
    weight_place = P('ep', None, None)
    slot_place = P('dp', 'ep', None, None)
    grad_place = P(('dp', 'ep'), None, None)
    return jax.shard_map(local_step, mesh=mesh,
                         in_specs=(slot_place, weight_place, weight_place, weight_place, token_place, token_place, token_place, token_place),
                         out_specs=(slot_place, grad_place, grad_place, grad_place, token_place),
                         check_vma=False)
```

```python
import functools

import jax
import jax.numpy as jnp
from jax import lax
from jax.experimental import pallas as pl
from jax.experimental.pallas import tpu as pltpu
from jax.sharding import PartitionSpec as P

BF16 = jnp.bfloat16
F32 = jnp.float32
MESH = pl.DeviceIdType.MESH
NT = (((1,), (1,)), ((), ()))
TN = (((0,), (0,)), ((), ()))
PASS_AT = 6
FAR_AT = 5
TILE_M = 192


def slot_kernel(x_hbm, wg_hbm, wu_hbm, wd_hbm, d_hbm, slot_in, exp_in, gate_in,
                mix_hbm, gg_out, cnt_ref,
                d_all, f1, f2, hid, m_all, gg, gg_in, xb, wgb, wub, wdb, dbuf, abb,
                x_sem, w_sem, wd_sem, own_sem, h_sem, out_sem,
                link_send, link_recv, meta_send, meta_recv, gg_send, gg_recv):
    chips, cores = 4, 2
    n_dev = chips * cores
    e_local, cap = x_hbm.shape[1], x_hbm.shape[2]
    tok, dim, ffn = d_hbm.shape[0], d_hbm.shape[1], wg_hbm.shape[2]
    top_k = slot_in.shape[0]
    half = tok // 2
    quad = n_dev // 2
    blocks = 2 * e_local
    ab_hbm = mix_hbm.at[:, :, :, :2 * ffn]
    dy_hbm = mix_hbm.at[:, :, :, 2 * ffn:2 * ffn + dim]
    h_hbm = mix_hbm.at[:, :, :, 2 * ffn + dim:]
    me = lax.axis_index('ep')
    chip, core = me // cores, me % cores
    right = lax.rem(chip + 1, chips)
    left = lax.rem(chip + chips - 1, chips)
    far = lax.rem(chip + 2, chips)
    to_right, to_left, to_sib = right * cores + core, left * cores + core, chip * cores + (1 - core)

    def x_copies(i, slot):
        return [pltpu.make_async_copy(x_hbm.at[(i % 2) * quad + k, i // 2], xb.at[slot, pl.ds(k * cap, cap)], x_sem.at[slot, k])
                for k in range(quad)]

    def w_copies(e, slot):
        return (pltpu.make_async_copy(wg_hbm.at[e], wgb.at[slot], w_sem.at[slot, 0]),
                pltpu.make_async_copy(wu_hbm.at[e], wub.at[slot], w_sem.at[slot, 1]))

    def h_copies(i):
        return [pltpu.make_async_copy(hid.at[i, pl.ds(k * cap, cap)], h_hbm.at[(i % 2) * quad + k, i // 2], h_sem.at[i, k])
                for k in range(quad)]

    def rows(h):
        return pl.ds(h * half, half)

    def link(src_ref, s, h, dst, n):
        return pltpu.make_async_remote_copy(src_ref=src_ref, dst_ref=d_all.at[s, rows(h)], send_sem=link_send.at[n],
                                            recv_sem=link_recv.at[s, h], device_id={'ep': dst}, device_id_type=MESH)

    def meta(s, dst, n):
        return pltpu.make_async_remote_copy(src_ref=m_all.at[s], dst_ref=m_all.at[s], send_sem=meta_send.at[n],
                                            recv_sem=meta_recv.at[s], device_id={'ep': dst}, device_id_type=MESH)

    def gg_copy(other, s):
        return pltpu.make_async_remote_copy(src_ref=gg.at[other], dst_ref=gg_in.at[s], send_sem=gg_send.at[other],
                                            recv_sem=gg_recv.at[s], device_id={'ep': other}, device_id_type=MESH)

    def got(s, h):
        link(d_hbm.at[rows(h)], s, h, to_sib, 0).wait_recv()

    def peers(do):
        def step(k, carry):
            do(lax.rem(me + k, n_dev))
            return carry
        lax.fori_loop(1, n_dev, step, 0)

    m_all[me, :top_k] = slot_in[...].astype(F32)
    m_all[me, top_k:2 * top_k] = exp_in[...].astype(F32)
    m_all[me, 2 * top_k:] = gate_in[...]
    barrier = pltpu.get_barrier_semaphore()
    peers(lambda other: pl.semaphore_signal(barrier, inc=1, device_id={'ep': other}, device_id_type=MESH))
    for c in x_copies(0, 0):
        c.start()
    for c in w_copies(0, 0):
        c.start()
    own_copy = pltpu.make_async_copy(d_hbm, d_all.at[me], own_sem)
    own_copy.start()
    wd_copy = pltpu.make_async_copy(wd_hbm, wdb, wd_sem)
    pl.semaphore_wait(barrier, n_dev - 1)

    own_links = [link(d_hbm.at[rows(h)], me, h, dst, n) for n, (dst, h) in enumerate(
        ((to_right, 0), (to_left, 1), (to_right, 1), (to_left, 0), (to_sib, 0), (to_sib, 1)))]
    to_far = far * cores + core
    own_meta = [meta(me, dst, n) for n, dst in enumerate((to_right, to_left, to_far, to_sib))]
    for c in own_meta + own_links:
        c.start()
    wd_copy.start()

    l_src, r_src, f_src = left * cores + core, right * cores + core, far * cores + core
    pass_on = [link(d_all.at[l_src, rows(0)], l_src, 0, to_right, 6), link(d_all.at[r_src, rows(1)], r_src, 1, to_left, 7)]
    share = [link(d_all.at[s, rows(h)], s, h, to_sib, 8 + n) for n, (s, h) in enumerate(
        ((l_src, 0), (r_src, 1), (r_src, 0), (l_src, 1), (f_src, 0), (f_src, 1)))]

    share_meta = [meta(s, to_sib, 4 + n) for n, s in enumerate((l_src, r_src, f_src))]

    def forward(i, carry):
        slot = i % 2
        e = i // 2

        @pl.when(i + 1 < blocks)
        def _():
            for c in x_copies(i + 1, 1 - slot):
                c.start()

        @pl.when(i % 2 == 0)
        def _():
            for c in w_copies(e, e % 2):
                c.wait()

            @pl.when(e + 1 < e_local)
            def _():
                for c in w_copies(e + 1, (e + 1) % 2):
                    c.start()

        for c in x_copies(i, slot):
            c.wait()

        @pl.when(i == 3)
        def _():
            for n, s in enumerate((l_src, r_src, f_src)):
                meta(s, to_sib, 0).wait_recv()
                share_meta[n].start()

        @pl.when(i == PASS_AT)
        def _():
            got(l_src, 0)
            pass_on[0].start()
            got(r_src, 1)
            pass_on[1].start()

        for m in range(0, quad * cap, TILE_M):
            x = xb[slot, m:m + TILE_M]
            for n in range(0, ffn, 256):
                a = jnp.dot(x, wgb[e % 2, :, n:n + 256], preferred_element_type=F32)
                b = jnp.dot(x, wub[e % 2, :, n:n + 256], preferred_element_type=F32)
                sg = jax.nn.sigmoid(a)
                silu = a * sg
                f1[i, m:m + TILE_M, n:n + 256] = b * sg * (1.0 + a * (1.0 - sg))
                f2[i, m:m + TILE_M, n:n + 256] = silu
                hid[i, m:m + TILE_M, n:n + 256] = (silu * b).astype(BF16)
        for c in h_copies(i):
            c.start()
        return carry

    lax.fori_loop(0, blocks, forward, 0)

    own_copy.wait()
    wd_copy.wait()

    for s in (to_sib, left * cores + 1 - core, right * cores + 1 - core, far * cores + 1 - core):
        meta(s, to_sib, 0).wait_recv()
    got(to_sib, 0)
    got(to_sib, 1)

    cap_ids = lax.broadcasted_iota(jnp.int32, (cap, tok), 0).astype(F32)

    def sources(g):
        near = ((g + 1) // 2) % 2
        c = (core + g // 2) % 2
        first = near * (left * cores + c) + (1 - near) * (lax.rem(chip + 2 * (g // 2), chips) * cores)
        second = near * (right * cores + c) + (1 - near) * (lax.rem(chip + 2 * (g // 2), chips) * cores + 1)
        return first, second

    def out_copies(j, slot):
        return [pltpu.make_async_copy(buf.at[slot, pl.ds((v * cores + k) * cap, cap)], dst.at[s, (j % 2) * 2 + v], out_sem.at[slot, a, v, k])
                for a, (buf, dst) in enumerate(((xb, dy_hbm), (abb, ab_hbm))) for v in range(2) for k, s in enumerate(sources(j // 2))]

    def backward(j, carry):
        slot = j % 2
        g = j // 2
        pair = sources(g)

        @pl.when(j == 2)
        def _():
            got(r_src, 0)
            got(l_src, 1)
            for c in share[:4]:
                c.start()

        @pl.when(j == 4)
        def _():
            for s in (right * cores + 1 - core, left * cores + 1 - core):
                got(s, 0)
                got(s, 1)

        @pl.when(j == FAR_AT)
        def _():
            got(f_src, 0)
            share[4].start()
            got(f_src, 1)
            share[5].start()

        @pl.when(j == 6)
        def _():
            for h in range(2):
                got(far * cores + 1 - core, h)

        @pl.when(j >= 2)
        def _():
            for c in out_copies(j - 2, slot):
                c.wait()

        hits, gates = [], []
        for k, s in enumerate(pair):
            for v in range(2):
                e = (j % 2) * 2 + v
                slots = m_all[s, :top_k]
                match = (m_all[s, top_k:2 * top_k] == (me * e_local + e).astype(F32)) & (slots >= 0.0)
                at = jnp.sum(jnp.where(match, slots + 1.0, 0.0), axis=0, keepdims=True) - 1.0
                gate = jnp.sum(jnp.where(match, m_all[s, 2 * top_k:], 0.0), axis=0, keepdims=True)
                cnt_ref[s * e_local + e] = jnp.sum(jnp.where(match, 1, 0))
                hit = cap_ids == at
                hits.append(hit)
                gates.append(jnp.sum(jnp.where(hit, gate, 0.0), axis=1, keepdims=True))
        for k, s in enumerate(pair):
            pick = jnp.concatenate([jnp.where(hits[k * 2 + v], 1.0, 0.0).astype(BF16) for v in range(2)], axis=0)
            for n in range(0, dim, 256):
                d = jnp.dot(pick, d_all[s, :, n:n + 256], preferred_element_type=F32)
                for v in range(2):
                    at = (v * cores + k) * cap
                    dv = d[v * cap:(v + 1) * cap]
                    dbuf[at:at + cap, n:n + 256] = dv.astype(BF16)
                    xb[slot, at:at + cap, n:n + 256] = (dv * gates[k * 2 + v]).astype(BF16)
        for v in range(2):
            e = (j % 2) * 2 + v
            top = v * cores * cap
            dots = [jnp.zeros((cap, 1), F32) for _ in pair]
            for n in range(0, ffn, 256):
                u2 = lax.dot_general(dbuf[top:top + cores * cap], wdb[e, n:n + 256, :], NT, preferred_element_type=F32)
                for k, s in enumerate(pair):
                    i = e * 2 + s // quad
                    at = pl.ds(pl.multiple_of((s % quad) * cap, cap), cap)
                    u = u2[k * cap:(k + 1) * cap]
                    dots[k] = dots[k] + jnp.sum(u * hid[i, at, n:n + 256].astype(F32), axis=1, keepdims=True)
                    dh = (u * gates[k * 2 + v]).astype(BF16).astype(F32)
                    to = pl.ds(top + k * cap, cap)
                    abb[slot, to, n:n + 256] = (dh * f1[i, at, n:n + 256]).astype(BF16)
                    abb[slot, to, ffn + n:ffn + n + 256] = (dh * f2[i, at, n:n + 256]).astype(BF16)
            for k, s in enumerate(pair):
                gg[s, e] = jnp.sum(jnp.where(hits[k * 2 + v], dots[k], 0.0), axis=0, keepdims=True)
        for c in out_copies(j, slot):
            c.start()

        @pl.when((j % 2 == 1) & (j > 1))
        def _():
            for s in pair:
                gg_copy(s, me).start()

        @pl.when(j == 1)
        def _():
            gg_copy(to_sib, me).start()
        return carry

    lax.fori_loop(0, blocks, backward, 0)
    for j in (blocks - 2, blocks - 1):
        for c in out_copies(j, j % 2):
            c.wait()

    def h_done(i, carry):
        for c in h_copies(i):
            c.wait()
        return carry
    lax.fori_loop(0, blocks, h_done, 0)

    def sent(other):
        gg_copy(other, me).wait_send()
    peers(sent)
    for c in own_meta + share_meta + own_links + pass_on + share:
        c.wait_send()
    gg_in[me] = gg[me]
    peers(lambda s: gg_copy(s, s).wait_recv())
    gg_out[...] = gg_in[...]


def slot_call(x_disp, w_gate, w_up, w_down, d_out, slot_t, exp_t, gate_t):
    n_src, e_local, cap, dim = x_disp.shape
    ffn = w_gate.shape[2]
    tok, top_k = d_out.shape[0], slot_t.shape[0]
    blocks, quad = 2 * e_local, n_src // 2
    hbm = pl.BlockSpec(memory_space=pl.ANY)
    vmem = pl.BlockSpec(memory_space=pltpu.VMEM)
    smem = pl.BlockSpec(memory_space=pltpu.SMEM)
    dma = pltpu.SemaphoreType.DMA
    return pl.pallas_call(
        slot_kernel,
        out_shape=(jax.ShapeDtypeStruct((n_src, e_local, cap, 3 * ffn + dim), BF16),
                   jax.ShapeDtypeStruct((n_src, e_local, 1, tok), F32),
                   jax.ShapeDtypeStruct((n_src * e_local,), jnp.int32)),
        in_specs=[hbm] * 5 + [vmem] * 3,
        out_specs=(hbm, vmem, smem),
        scratch_shapes=[
            pltpu.VMEM((n_src, tok, dim), BF16),
            pltpu.VMEM((blocks, quad * cap, ffn), F32), pltpu.VMEM((blocks, quad * cap, ffn), F32),
            pltpu.VMEM((blocks, quad * cap, ffn), BF16),
            pltpu.VMEM((n_src, 3 * top_k, tok), F32),
            pltpu.VMEM((n_src, e_local, 1, tok), F32), pltpu.VMEM((n_src, e_local, 1, tok), F32),
            pltpu.VMEM((2, quad * cap, dim), BF16),
            pltpu.VMEM((2, dim, ffn), BF16), pltpu.VMEM((2, dim, ffn), BF16), pltpu.VMEM((e_local, ffn, dim), BF16),
            pltpu.VMEM((quad * cap, dim), BF16), pltpu.VMEM((2, quad * cap, 2 * ffn), BF16),
            dma((2, quad)), dma((2, 2)), dma, dma, dma((blocks, quad)), dma((2, 2, 2, 2)),
            dma((14,)), dma((n_src, 2)), dma((7,)), dma((n_src,)), dma((n_src,)), dma((n_src,)),
        ],
        compiler_params=pltpu.CompilerParams(collective_id=0, has_side_effects=True, vmem_limit_bytes=62 * 1024 * 1024),
        cost_estimate=pl.CostEstimate(flops=8 * n_src * e_local * cap * dim * ffn, bytes_accessed=64 * 2 ** 20, transcendentals=0),
        name='slot_cotangents',
    )(x_disp, w_gate, w_up, w_down, d_out, slot_t, exp_t, gate_t)


def grad_kernel(cnt, x_hbm, mix_hbm, wg_hbm, wu_hbm, gg, exp_in,
                dx_hbm, dwg_hbm, dwu_hbm, dwd_hbm, gate_out,
                xb, mixb, wgb, wub, dxb, dwgb, dwub, dwdb, zeros,
                in_sem, w_sem, dx_sem, z_sem, dw_sem):
    n_src, e_local, cap, dim = x_hbm.shape
    ffn = wg_hbm.shape[2]
    step, grain = 256, 16
    pairs = ((x_hbm, xb), (mix_hbm, mixb))
    dy_at, h_at = 2 * ffn, 2 * ffn + dim

    def spans(e):
        out, start = [], jnp.int32(0)
        for s in range(n_src):
            n = (cnt[s * e_local + e] + (grain - 1)) // grain * grain
            out.append((pl.multiple_of(start, grain), pl.multiple_of(n, grain)))
            start = start + n
        return out, pl.multiple_of(start, grain)

    def loads(e, slot, which, do):
        for j in which:
            if j == 2:
                do(pltpu.make_async_copy(wg_hbm.at[e], wgb.at[slot], w_sem.at[slot, 0]))
                do(pltpu.make_async_copy(wu_hbm.at[e], wub.at[slot], w_sem.at[slot, 1]))
                continue
            src, dst = pairs[j]
            for s, (start, n) in enumerate(spans(e)[0]):
                do(pltpu.make_async_copy(src.at[s, e, pl.ds(0, n)], dst.at[slot, pl.ds(start, n)], in_sem.at[slot, j, s]))

    def dx_stores(e, slot, do):
        for s, (start, n) in enumerate(spans(e)[0]):
            do(pltpu.make_async_copy(dxb.at[slot, pl.ds(start, n)], dx_hbm.at[s, e, pl.ds(0, n)], dx_sem.at[slot, s]))

    def zero_stores(e, do):
        for s, (_, n) in enumerate(spans(e)[0]):
            rest = pl.multiple_of(cap - n, grain)
            do(pltpu.make_async_copy(zeros.at[pl.ds(0, rest)], dx_hbm.at[s, e, pl.ds(n, rest)], z_sem.at[s]))

    def dw_stores(e, slot, which, do):
        for j in which:
            src, dst = ((dwgb, dwg_hbm), (dwub, dwu_hbm), (dwdb, dwd_hbm))[j]
            do(pltpu.make_async_copy(src.at[slot], dst.at[e], dw_sem.at[slot, j]))

    start = lambda c: c.start()
    wait = lambda c: c.wait()

    order = (2, 1, 0)
    loads(0, 0, order, start)
    zeros[...] = jnp.zeros_like(zeros)
    ids = exp_in[...]
    gate_out[...] = sum(jnp.where(ids == s * e_local + e, gg[s, e], 0.0) for s in range(n_src) for e in range(e_local))

    def expert(e, carry):
        slot = e % 2

        @pl.when(e + 1 < e_local)
        def _():
            loads(e + 1, 1 - slot, order, start)

        @pl.when(e > 0)
        def _():
            zero_stores(e - 1, wait)
        zero_stores(e, start)
        loads(e, slot, (2, 1), wait)

        @pl.when(e >= 2)
        def _():
            dx_stores(e - 2, slot, wait)
            dw_stores(e - 2, slot, (0, 1, 2), wait)

        total = spans(e)[1]
        count = jnp.maximum((total + (step - 1)) // step, 1)

        def clear(j, c):
            at = pl.ds(pl.multiple_of(total + j * grain, grain), grain)
            for buf in (xb, mixb):
                buf[slot, at, :] = jnp.zeros((grain, buf.shape[2]), BF16)
            return c
        lax.fori_loop(0, (count * step - total) // grain, clear, 0)

        def by_count(tiles):
            for k in range(1, n_src * cap // step + 1):
                @pl.when(count == k)
                def _():
                    tiles(k * step)

        def dx_tiles(rows):
            for n in range(0, dim, 256):
                dxb[slot, :rows, n:n + 256] = (
                    lax.dot_general(mixb[slot, :rows, :ffn], wgb[slot, n:n + 256, :], NT, preferred_element_type=F32)
                    + lax.dot_general(mixb[slot, :rows, ffn:dy_at], wub[slot, n:n + 256, :], NT, preferred_element_type=F32)).astype(BF16)

        def up_tiles(rows):
            for n in range(0, dim, 256):
                up = lax.dot_general(xb[slot, :rows, n:n + 256], mixb[slot, :rows, :dy_at], TN, preferred_element_type=F32).astype(BF16)
                dwgb[slot, n:n + 256, :] = up[:, :ffn]
                dwub[slot, n:n + 256, :] = up[:, ffn:]

        def down_tiles(rows):
            for n in range(0, ffn, 256):
                dwdb[slot, n:n + 256, :] = lax.dot_general(mixb[slot, :rows, h_at + n:h_at + n + 256], mixb[slot, :rows, dy_at:h_at], TN, preferred_element_type=F32).astype(BF16)

        by_count(dx_tiles)
        dx_stores(e, slot, start)
        loads(e, slot, (0,), wait)
        by_count(up_tiles)
        dw_stores(e, slot, (0, 1), start)
        by_count(down_tiles)
        dw_stores(e, slot, (2,), start)
        return carry

    lax.fori_loop(0, e_local, expert, 0)
    zero_stores(e_local - 1, wait)
    for e in range(max(e_local - 2, 0), e_local):
        dx_stores(e, e % 2, wait)
        dw_stores(e, e % 2, (0, 1, 2), wait)


def grad_call(cnt, x_disp, mix, w_gate, w_up, gg, exp_t):
    n_src, e_local, cap, dim = x_disp.shape
    ffn = w_gate.shape[2]
    most = n_src * cap
    hbm = pl.BlockSpec(memory_space=pl.ANY)
    vmem = pl.BlockSpec(memory_space=pltpu.VMEM)
    dma = pltpu.SemaphoreType.DMA
    return pl.pallas_call(
        grad_kernel,
        out_shape=(jax.ShapeDtypeStruct(x_disp.shape, BF16), jax.ShapeDtypeStruct(w_gate.shape, BF16),
                   jax.ShapeDtypeStruct(w_up.shape, BF16), jax.ShapeDtypeStruct((e_local, ffn, dim), BF16), jax.ShapeDtypeStruct(exp_t.shape, F32)),
        in_specs=[pl.BlockSpec(memory_space=pltpu.SMEM)] + [hbm] * 4 + [vmem] * 2,
        out_specs=(hbm,) * 4 + (vmem,),
        scratch_shapes=[
            pltpu.VMEM((2, most, dim), BF16), pltpu.VMEM((2, most, 3 * ffn + dim), BF16),
            pltpu.VMEM((2, dim, ffn), BF16), pltpu.VMEM((2, dim, ffn), BF16),
            pltpu.VMEM((2, most, dim), BF16),
            pltpu.VMEM((2, dim, ffn), BF16), pltpu.VMEM((2, dim, ffn), BF16), pltpu.VMEM((2, ffn, dim), BF16),
            pltpu.VMEM((cap, dim), BF16),
            dma((2, 2, n_src)), dma((2, 2)), dma((2, n_src)), dma((n_src,)), dma((2, 3)),
        ],
        compiler_params=pltpu.CompilerParams(vmem_limit_bytes=62 * 1024 * 1024),
        cost_estimate=pl.CostEstimate(flops=10 * n_src * e_local * cap * dim * ffn, bytes_accessed=64 * 2 ** 20, transcendentals=0),
        name='slot_gradients',
    )(cnt, x_disp, mix, w_gate, w_up, gg, exp_t)


def solution(mesh):
    def local_step(x_disp, w_gate, w_up, w_down, d_out, slot_idx, expert_id, gate_wt):
        exp_t = expert_id.T
        mix, gg, cnt = slot_call(x_disp, w_gate, w_up, w_down, d_out, slot_idx.T, exp_t, gate_wt.T)
        grad_x, grad_wg, grad_wu, grad_wd, gate_t = grad_call(cnt, x_disp, mix, w_gate, w_up, gg, exp_t)
        return grad_x, grad_wg, grad_wu, grad_wd, gate_t.T

    token_place = P(('dp', 'ep'), None)
    weight_place = P('ep', None, None)
    slot_place = P('dp', 'ep', None, None)
    grad_place = P(('dp', 'ep'), None, None)
    return jax.shard_map(local_step, mesh=mesh,
                         in_specs=(slot_place, weight_place, weight_place, weight_place, token_place, token_place, token_place, token_place),
                         out_specs=(slot_place, grad_place, grad_place, grad_place, token_place),
                         check_vma=False)
```
